32 devices in a mesh: slab: 8 (over y, x, core), lev: 4 (over z).
Axes of the slice: x: 2, y: 2, z: 4, core: 2. Of those that a mesh axis runs over, the one named last changes fastest.
Arguments:
- ensemble: float32 [80, 16, 18432], P(None, 'lev', 'slab'), may hold values from -6 to 6
- obs_cell: int32 [2, 256], replicated, may hold values from 0 to 294911, as said below
- obs_value: float32 [2, 256], replicated, may hold values from -6 to 6
- obs_var: float32 [2, 256], replicated, may hold values from 0.3 to 3
- obs_frac: float32 [2, 256], replicated, may hold values from 0 to 1
- loc_column: bfloat16 [2, 256, 18432], P(None, 'lev', 'slab'), may hold values from 0 to 1
- loc_level: float32 [2, 256, 16], P(None, None, 'lev'), may hold values from 0.2 to 1
Outputs:
- analysis: float32 [80, 16, 18432], P(None, 'lev', 'slab')
- prior_mean: float32 [2, 256], replicated
The draws below stay inside these ranges and needn't reach their ends.
Inputs may be any that keep to these rules, and one draw needn't show every extreme that they name: `obs_cell`: in each block, every device's cells (a level band of 4 levels and a slab of 2304 columns) hold at least one observation, and one of them lies in the slab's last column.
All inputs are finite; a program needn't handle non-finite values.
Results may differ from the reference program's by a relative error of at most 0.0055.
Values may be sent and summed in bfloat16 or wider, within the bound.
A program may use at most 64 MiB of HBM per device.

```python
import math
import jax
import jax.numpy as jnp
from jax import lax

MEM = 80
CL = 4
CC = 2304
NOBS = 256
BLOCKS = 2
NL = 16
NC = 18432


def draw_obs_cell(key, part):
    n_slabs = NC // CC
    n_bands = NL // CL
    owners = n_slabs * n_bands
    block_rows = []
    for block_index in range(BLOCKS):
        block_key = jax.random.fold_in(key, 101 + block_index)
        keys = jax.random.split(block_key, 6)
        owner_ids = jax.random.permutation(keys[0], owners).astype(jnp.int32)
        owner_slab = owner_ids % n_slabs
        owner_band = owner_ids // n_slabs
        owner_level = owner_band * CL + jax.random.randint(keys[1], (owners,), 0, CL, dtype=jnp.int32)
        owner_column = owner_slab * CC + CC - 1
        extra = NOBS - owners
        rest_level = jax.random.randint(keys[2], (extra,), 0, NL, dtype=jnp.int32)
        slab_one = jax.random.randint(keys[3], (extra,), 0, n_slabs, dtype=jnp.int32)
        slab_two = jax.random.randint(keys[4], (extra,), 0, n_slabs, dtype=jnp.int32)
        rest_slab = slab_one * slab_two // n_slabs
        rest_column = rest_slab * CC + jax.random.randint(keys[5], (extra,), 0, CC, dtype=jnp.int32)
        levels_all = jnp.concatenate([owner_level, rest_level])
        columns_all = jnp.concatenate([owner_column, rest_column])
        block_rows.append((levels_all * NC + columns_all).astype(jnp.int32))
    return jnp.stack(block_rows)


def steps_of(own_key, dims, cuts, smallest, largest):
    def one(position, shards_of):
        steps = jax.random.uniform(jax.random.fold_in(jax.random.fold_in(own_key, 6), position), (shards_of,), jnp.float32, smallest / len(cuts), largest / len(cuts))
        return jnp.repeat(jnp.exp(steps), dims[position] // shards_of).reshape((-1,) + (1,) * (len(dims) - position - 1))

    factor_of = one(*cuts[0])
    for cut in cuts[1:]:
        factor_of = factor_of * one(*cut)
    return factor_of


def scatter_about(key, shape, scale, reach, cuts=(), kind=jnp.bfloat16):
    gain = steps_of(key, shape, cuts, -0.22, 0.18) if cuts else 1.0
    array = jax.random.normal(key, shape, jnp.float32) * scale * gain
    return jnp.minimum(jnp.maximum(array, -reach), reach).astype(kind)


def setup_inputs(seed: int = 0) -> dict:
    seeds = jax.random.split(jax.random.key(seed), 8)
    ensemble = scatter_about(seeds[0], (MEM, NL, NC), 1.0, 6.0, ((1, 4), (2, 8)), jnp.float32)
    obs_cell = draw_obs_cell(jax.random.fold_in(seeds[7], 71), 0)
    obs_value = scatter_about(seeds[2], (BLOCKS, NOBS), 1.5, 6.0, (), jnp.float32)
    obs_var = jnp.clip(jnp.exp(jax.random.uniform(seeds[3], (BLOCKS, NOBS), jnp.float32, math.log(0.3), math.log(3.0))), 0.3, 3.0)
    obs_frac = jnp.clip(jax.random.uniform(seeds[4], (BLOCKS, NOBS), jnp.float32, 0.0, 1.0), 0.0, 1.0)
    loc_column = jnp.clip(1.0 * jax.random.uniform(seeds[5], (BLOCKS, NOBS, NC), jnp.float32) ** steps_of(seeds[5], (BLOCKS, NOBS, NC), ((1, 4), (2, 8)), -0.2, 0.2), 0.0, 1.0).astype(jnp.bfloat16)
    loc_level = jnp.clip(0.2 + 0.8 * jax.random.uniform(seeds[6], (BLOCKS, NOBS, NL), jnp.float32) ** steps_of(seeds[6], (BLOCKS, NOBS, NL), ((2, 4),), -0.2, 0.2), 0.2, 1.0)
    return dict(ensemble=ensemble, obs_cell=obs_cell, obs_value=obs_value, obs_var=obs_var, obs_frac=obs_frac, loc_column=loc_column, loc_level=loc_level)


def obs_stats(prior_obs, obs_val, variance):
    members = prior_obs.shape[1]
    obs_mean = lax.optimization_barrier(jnp.mean(prior_obs, axis=1))
    deviation = prior_obs - obs_mean[:, None]
    spread = lax.optimization_barrier(jnp.sum(deviation * deviation, axis=1)) / (members - 1.0)
    total_var = spread + variance
    shrink = 1.0 / (1.0 + jnp.sqrt(variance / total_var))
    gain_rows = ((obs_val - obs_mean)[:, None] - deviation * shrink[:, None]) / (total_var * (members - 1.0))[:, None]
    return (obs_mean, deviation.astype(jnp.bfloat16), gain_rows.astype(jnp.bfloat16))

def reference(ensemble, obs_cell, obs_value, obs_var, obs_frac, loc_column, loc_level):
    current = ensemble
    prior_means = []
    for block_index in range(BLOCKS):
        obs_cells = obs_cell[block_index]
        obs_level = obs_cells // NC
        obs_column = obs_cells % NC
        next_column = (obs_column + 1) % NC
        flattened = current.reshape(MEM, NL * NC)
        first_val = jnp.take(flattened, obs_level * NC + obs_column, axis=1)
        second = jnp.take(flattened, obs_level * NC + next_column, axis=1)
        fraction = obs_frac[block_index]
        prior_obs = ((1.0 - fraction)[None, :] * first_val + fraction[None, :] * second).T
        obs_mean, dev_b, gain_b = obs_stats(prior_obs, obs_value[block_index], obs_var[block_index])
        prior_means.append(obs_mean)
        centred = (current - lax.optimization_barrier(jnp.mean(current, axis=0))).astype(jnp.bfloat16)
        col_weights = loc_column[block_index]
        lev_weights = loc_level[block_index]

        def level_step(level_index):
            level_slab = lax.dynamic_index_in_dim(centred, level_index, 1, keepdims=False)
            level_loc = lax.dynamic_index_in_dim(lev_weights, level_index, 1, keepdims=False)
            cross_cov = jnp.dot(dev_b, level_slab, preferred_element_type=jnp.float32)
            mixed_rows = (level_loc[:, None] * col_weights.astype(jnp.float32) * cross_cov).astype(jnp.bfloat16)
            return jnp.dot(gain_b.T, mixed_rows, preferred_element_type=jnp.float32)
        increment = lax.map(level_step, jnp.arange(NL, dtype=jnp.int32))
        current = current + jnp.transpose(increment, (1, 0, 2))
    return (current, jnp.stack(prior_means))
```

```python
import functools

import jax
import jax.numpy as jnp
from jax import lax
from jax.experimental import pallas as pl
from jax.experimental.pallas import tpu as pltpu
from jax.sharding import PartitionSpec as P

MESH = pl.DeviceIdType.MESH
LANES = 128
SUBLANES = 8
F32 = jnp.float32
BF16 = jnp.bfloat16
SKEW = 3
STEPS_FIRST = (1, 2, 1)
STEPS_LATER = (2, 3, 2)


def kernel(
    n_slab, n_lev, cell_ref, frac_ref, value_ref, var_ref, lev_ref, ens_hbm, loc_hbm, out_ref, mean_ref,
    raw, plain, gat, keys, acc, part, landed, zown, zland, own, prior, dev_s, gain_s, lev_s,
    load_sem, line_recv, first_send, line_send, scat_send, scat_recv, z_send, z_recv, cast_send, cast_recv, out_sem,
):
    members, lev_rows, cols = raw.shape
    n_blocks, n_obs = cell_ref.shape
    rows = loc_hbm.shape[1]
    tiles = cols // LANES
    chunks = line_recv.shape[2]
    width = cols // chunks
    wide = width // LANES
    total = cols * n_slab
    slots = n_obs // n_slab
    lag = SKEW * (n_lev - 2)
    steps = chunks + lag
    obs_tiles = n_obs // LANES
    slab, lev = lax.axis_index("slab"), lax.axis_index("lev")

    loads = [
        pltpu.make_async_copy(loc_hbm.at[b], gat.at[b, pl.ds(pl.multiple_of(lev * rows, rows), rows), :], load_sem.at[b])
        for b in range(n_blocks)
    ]
    loads.append(pltpu.make_async_copy(ens_hbm, raw, load_sem.at[n_blocks]))
    for load in loads:
        load.start()

    def on_slab(k):
        p = lax.rem(slab + k, n_slab)
        return p, (p, lev)

    def on_line(k):
        return (slab, lax.rem(lev + k, n_lev))

    barrier = pltpu.get_barrier_semaphore()
    for k in range(1, n_lev):
        pl.semaphore_signal(barrier, inc=1, device_id=on_line(k), device_id_type=MESH)
    for k in range(1, n_slab):
        pl.semaphore_signal(barrier, inc=1, device_id=on_slab(k)[1], device_id_type=MESH)
    pl.semaphore_wait(barrier, n_slab + n_lev - 2)

    def hop(step, b, source, c, sem):
        spot = gat.at[
            b, pl.ds(pl.multiple_of(source * rows, rows), rows), pl.ds(pl.multiple_of(c * width, width), width)
        ]
        return pltpu.make_async_remote_copy(
            src_ref=spot, dst_ref=spot, send_sem=sem, recv_sem=line_recv.at[b, source, c],
            device_id=(slab, lev + step), device_id_type=MESH)

    ends = ((0, 1, lev < n_lev - 1), (1, -1, lev > 0))

    def send_own_first(c, carry):
        for way, step, alive in ends:
            @pl.when(alive)
            def _():
                hop(step, 0, lev, c, first_send.at[way, c]).start()
        return carry

    loads[0].wait()
    lax.fori_loop(0, chunks, send_own_first, 0)

    def send(way, step, d, b, source, c, order):
        sem = line_send.at[way, d, lax.rem(order, 2)]

        @pl.when(order >= 2)
        def _():
            hop(step, b, source, c, sem).wait_send()

        hop(step, b, source, c, sem).start()

    def forward(b, s):
        if b + 1 < n_blocks:
            pass
        for d in range(1, n_lev):
            c = s - (d - 1) * SKEW

            @pl.when((c >= 0) & (c < chunks))
            def _():
                for way, step, alive in ends:
                    source = lev - step * d

                    @pl.when((source >= 0) & (source < n_lev))
                    def _():
                        hop(step, b, source, c, line_send.at[way, d, 0]).wait_recv()
                        if d < n_lev - 1:
                            @pl.when(alive)
                            def _():
                                send(way, step, d, b, source, c, c + b * chunks)

        for nxt in range(1, n_blocks):
            c = s + (b - nxt + 1) * steps - chunks

            @pl.when((c >= 0) & (c < chunks))
            def _():
                for way, step, alive in ends:
                    @pl.when(alive)
                    def _():
                        send(way, step, 0, nxt, lev, c, c + (nxt - 1) * chunks)

    def forwards(b, start, stop):
        def body(s, carry):
            forward(b, s)
            return carry
        lax.fori_loop(start, stop, body, 0)

    def locate(b):
        cell = jnp.broadcast_to(cell_ref[b : b + 1, :], (SUBLANES, n_obs))
        rest = cell - lev * (lev_rows * total)
        row = jnp.zeros_like(rest)
        for level in range(1, lev_rows):
            row = row + (rest >= level * total).astype(jnp.int32)
        col = rest - row * total
        following = jnp.where(col + 1 == total, 0, col + 1)
        in_band = (rest >= 0) & (rest < lev_rows * total)
        for i, where in enumerate((col, following)):
            local = where - slab * cols
            mine = in_band & (local >= 0) & (local < cols)
            local = jnp.where(mine, local, 0)
            window = row * tiles + lax.shift_right_logical(local, 7)
            window = jnp.where(mine, window, -1)
            lane = local & (LANES - 1)
            for t in range(obs_tiles):
                at = slice(t * LANES, (t + 1) * LANES)
                keys[b, i, t, 0] = window[:, at]
                keys[b, i, t, 1] = lane[:, at]

    for b in range(n_blocks):
        locate(b)

    def gather(b, windows):
        for i in range(2):
            for t in range(obs_tiles):
                at = slice(t * LANES, (t + 1) * LANES)
                now = acc[i, :, at]
                window = keys[b, i, t, 0]
                lane = jnp.concatenate([keys[b, i, t, 1]] * (members // SUBLANES), axis=0)
                for ident, load in windows:
                    hit = jnp.concatenate([(window == ident).astype(jnp.int32)] * (members // SUBLANES), axis=0)
                    got = jnp.take_along_axis(load(), lane, axis=1, mode="promise_in_bounds")
                    now = jnp.where(hit > 0, got, now)
                acc[i, :, at] = now

    def finish_pick(b):
        frac = frac_ref[b : b + 1, :]
        value = acc[0] * (1.0 - frac) + acc[1] * frac
        pad = jnp.zeros((LANES - members, LANES), F32)
        for t in range(obs_tiles):
            at = slice(t * LANES, (t + 1) * LANES)
            part[b, at, :] = jnp.concatenate([value[:, at], pad], axis=0).T

    def pick_first(c, carry):
        windows = []
        for level in range(lev_rows):
            for w in range(wide):
                tile = c * wide + w
                load = lambda level=level, tile=tile: raw[:, level, pl.ds(pl.multiple_of(tile * LANES, LANES), LANES)]
                windows.append((level * tiles + tile, load))
        gather(0, windows)
        return carry

    def scatter(b, k):
        p, where = on_slab(k)
        return pltpu.make_async_remote_copy(
            src_ref=part.at[b, pl.ds(pl.multiple_of(p * slots, slots), slots), :], dst_ref=landed.at[b, k],
            send_sem=scat_send.at[b, k], recv_sem=scat_recv.at[b, k], device_id=where, device_id_type=MESH)

    def along(b, k):
        return pltpu.make_async_remote_copy(
            src_ref=zown.at[b], dst_ref=zland.at[b, k],
            send_sem=z_send.at[b, k], recv_sem=z_recv.at[b, k], device_id=on_line(k), device_id_type=MESH)

    def cast(b, k):
        return pltpu.make_async_remote_copy(
            src_ref=own.at[b], dst_ref=prior.at[b, slab],
            send_sem=cast_send.at[b, k], recv_sem=cast_recv.at[b, k], device_id=on_slab(k)[1], device_id_type=MESH)

    def exchange(b, fills):
        at, stop = 0, 0
        for k in range(1, n_slab):
            scatter(b, k).start()
        forwards(b, 0, fills[0])
        value = part[b, pl.ds(pl.multiple_of(slab * slots, slots), slots), :]
        for k in range(1, n_slab):
            scatter(b, k).wait_recv()
        for k in range(1, n_slab):
            value = value + landed[b, k]
        zown[b] = value
        for k in range(1, n_lev):
            along(b, k).start()
        forwards(b, fills[0], fills[0] + fills[1])
        for k in range(1, n_lev):
            along(b, k).wait_recv()
        for k in range(1, n_lev):
            value = value + zland[b, k]
        own[b] = value
        for k in range(1, n_slab):
            cast(b, k).start()
        prior[b, slab] = value
        forwards(b, fills[0] + fills[1], sum(fills))
        for k in range(1, n_slab):
            cast(b, k).wait_recv()

    def statistics(b):
        def column(ref):
            return jnp.broadcast_to(ref[b : b + 1, :], (SUBLANES, n_obs)).T[:, :1]

        value, var = column(value_ref), column(var_ref)
        now = prior[b].reshape(n_obs, LANES)
        live = lax.broadcasted_iota(jnp.int32, now.shape, 1) < members
        mean = jnp.sum(jnp.where(live, now, 0.0), axis=1, keepdims=True) / members
        deviation = jnp.where(live, now - mean, 0.0)
        spread = jnp.sum(deviation * deviation, axis=1, keepdims=True) / (members - 1.0)
        whole = spread + var
        shrink = 1.0 / (1.0 + jnp.sqrt(var / whole))
        gain = ((value - mean) - deviation * shrink) / (whole * (members - 1.0))
        dev_s[...] = deviation.astype(BF16)
        gain_s[...] = gain.T.astype(BF16)
        mean_ref[b : b + 1, :] = jnp.broadcast_to(mean, (n_obs, LANES)).T[:1, :]

    def spread_levels(b):
        for level in range(lev_rows):
            lev_s[level] = jnp.broadcast_to(lev_ref[b, level : level + 1, :], (LANES, n_obs)).T

    def update(b, c):
        first, last = b == 0, b == n_blocks - 1
        at = pl.ds(pl.multiple_of(c * width, width), width)
        dev = dev_s[:, :members]
        gain = gain_s[:members, :]
        loc = gat[b, :, at].astype(F32)
        for level in range(lev_rows):
            now = raw[:, level, at] if first else plain[level, :, at]
            centred = (now - jnp.sum(now, axis=0, keepdims=True) / members).astype(BF16)
            cross = jnp.dot(dev, centred, preferred_element_type=F32)
            height = jnp.concatenate([lev_s[level]] * wide, axis=1)
            mixed = ((height * loc) * cross).astype(BF16)
            new = now + jnp.dot(gain, mixed, preferred_element_type=F32)
            if last:
                raw[:, level, at] = new
            else:
                plain[level, :, at] = new
        if last:
            pltpu.make_async_copy(raw.at[:, :, at], out_ref.at[:, :, at], out_sem.at[c]).start()
        else:
            windows = []
            for level in range(lev_rows):
                for w in range(wide):
                    tile = c * wide + w
                    load = lambda level=level, tile=tile: plain[level, :, pl.ds(pl.multiple_of(tile * LANES, LANES), LANES)]
                    windows.append((level * tiles + tile, load))
            gather(b + 1, windows)

    acc[...] = jnp.zeros_like(acc)
    for load in loads[1:]:
        load.wait()
    lax.fori_loop(0, chunks, pick_first, 0)
    finish_pick(0)
    for b in range(n_blocks):
        fills = STEPS_FIRST if b == 0 else STEPS_LATER
        spread_levels(b)
        exchange(b, fills)
        statistics(b)
        if b + 1 < n_blocks:
            acc[...] = jnp.zeros_like(acc)
        done = sum(fills)
        early = max(done - lag, 0)

        def catch_up(c, carry):
            update(b, c)
            return carry

        def body(s, carry):
            forward(b, s)
            update(b, s - lag)
            return carry

        if early:
            lax.fori_loop(0, early, catch_up, 0)
        if done < lag:
            forwards(b, done, lag)
        lax.fori_loop(lag + early, steps, body, 0)
        if b + 1 < n_blocks:
            finish_pick(b + 1)

    def drain_first(c, carry):
        for way, step, alive in ends:
            @pl.when(alive)
            def _():
                hop(step, 0, lev, c, first_send.at[way, c]).wait_send()
        pltpu.make_async_copy(
            raw.at[:, :, pl.ds(pl.multiple_of(c * width, width), width)],
            out_ref.at[:, :, pl.ds(pl.multiple_of(c * width, width), width)], out_sem.at[c]).wait()
        return carry

    lax.fori_loop(0, chunks, drain_first, 0)
    for way, step, alive in ends:
        @pl.when(alive)
        def _():
            for d in range(n_lev - 1):
                if d == 0 and n_blocks == 1:
                    continue
                source = lev - step * d

                @pl.when((source >= 0) & (source < n_lev))
                def _():
                    for slot in range(2):
                        hop(step, 0, source, 0, line_send.at[way, d, slot]).wait_send()
    for b in range(n_blocks):
        for k in range(1, n_slab):
            scatter(b, k).wait_send()
            cast(b, k).wait_send()
        for k in range(1, n_lev):
            along(b, k).wait_send()


def analyse(n_slab, n_lev, ensemble, cells, values, variances, fracs, locs, heights):
    members, lev_rows, cols = ensemble.shape
    n_blocks, n_obs = cells.shape
    rows = locs.shape[1]
    width = next(t * LANES for t in (2, 1) if cols % (t * LANES) == 0)
    chunks = cols // width
    slots = n_obs // n_slab
    vmem = pl.BlockSpec(memory_space=pltpu.VMEM)
    hbm = pl.BlockSpec(memory_space=pltpu.HBM)
    dma = pltpu.SemaphoreType.DMA
    return pl.pallas_call(
        functools.partial(kernel, n_slab, n_lev),
        out_shape=[
            jax.ShapeDtypeStruct(ensemble.shape, F32),
            jax.ShapeDtypeStruct(values.shape, F32),
        ],
        in_specs=[vmem, vmem, vmem, vmem, vmem, hbm, hbm],
        out_specs=[pl.BlockSpec(memory_space=pl.ANY), vmem],
        scratch_shapes=[
            pltpu.VMEM((members, lev_rows, cols), F32),
            pltpu.VMEM((lev_rows, members, cols), F32),
            pltpu.VMEM((n_blocks, n_obs, cols), BF16),
            pltpu.VMEM((n_blocks, 2, n_obs // LANES, 2, SUBLANES, LANES), jnp.int32),
            pltpu.VMEM((2, members, n_obs), F32),
            pltpu.VMEM((n_blocks, n_obs, LANES), F32),
            pltpu.VMEM((n_blocks, n_slab, slots, LANES), F32),
            pltpu.VMEM((n_blocks, slots, LANES), F32),
            pltpu.VMEM((n_blocks, n_lev, slots, LANES), F32),
            pltpu.VMEM((n_blocks, slots, LANES), F32),
            pltpu.VMEM((n_blocks, n_slab, slots, LANES), F32),
            pltpu.VMEM((n_obs, LANES), BF16),
            pltpu.VMEM((LANES, n_obs), BF16),
            pltpu.VMEM((lev_rows, n_obs, LANES), F32),
            dma((n_blocks + 1,)),
            dma((n_blocks, n_lev, chunks)),
            dma((2, chunks)),
            dma((2, n_lev, 2)),
            dma((n_blocks, n_slab)),
            dma((n_blocks, n_slab)),
            dma((n_blocks, n_lev)),
            dma((n_blocks, n_lev)),
            dma((n_blocks, n_slab)),
            dma((n_blocks, n_slab)),
            dma((chunks,)),
        ],
        compiler_params=pltpu.CompilerParams(collective_id=0, has_side_effects=True, vmem_limit_bytes=28 << 20),
        name="analyse",
    )(cells, fracs, values, variances, heights, ensemble, locs)


def solution(mesh):
    n_slab, n_lev = mesh.shape["slab"], mesh.shape["lev"]

    def on_device(ensemble, obs_cell, obs_value, obs_var, obs_frac, loc_column, loc_level):
        heights = loc_level.transpose(0, 2, 1)
        state, means = analyse(n_slab, n_lev, ensemble, obs_cell, obs_value, obs_var, obs_frac, loc_column, heights)
        return state, means

    in_specs = (
        P(None, "lev", "slab"), P(), P(), P(), P(),
        P(None, "lev", "slab"), P(None, None, "lev"),
    )
    return jax.shard_map(
        on_device, mesh=mesh, in_specs=in_specs,
        out_specs=(P(None, "lev", "slab"), P()), check_vma=False,
    )
```

```python
import functools

import jax
import jax.numpy as jnp
from jax import lax
from jax.experimental import pallas as pl
from jax.experimental.pallas import tpu as pltpu
from jax.sharding import PartitionSpec as P

MESH = pl.DeviceIdType.MESH
LANES = 128
SUBLANES = 8
F32 = jnp.float32
BF16 = jnp.bfloat16
SKEW = 3
STEPS_FIRST = (3,3,3)
STEPS_LATER = (3,3,3)


def kernel(
    n_slab, n_lev, cell_hbm, frac_hbm, value_hbm, var_hbm, lev_hbm, ens_hbm, loc_hbm, state, mean_ref,
    cell_ref, frac_ref, value_ref, var_ref, lev_ref, gat, keys, acc, part, landed, zown, zland, own, prior, dev_s, gain_s, lev_s,
    load_sem, line_recv, first_send, line_send, scat_send, scat_recv, z_send, z_recv, cast_send, cast_recv,
):
    lev_rows, members, cols = state.shape
    n_blocks, n_obs = cell_hbm.shape
    rows = loc_hbm.shape[1]
    tiles = cols // LANES
    chunks = line_recv.shape[2]
    width = cols // chunks
    wide = width // LANES
    total = cols * n_slab
    slots = n_obs // n_slab
    lag = SKEW * (n_lev - 2)
    steps = chunks + lag
    obs_tiles = n_obs // LANES
    slab, lev = lax.axis_index("slab"), lax.axis_index("lev")

    loads = [
        pltpu.make_async_copy(loc_hbm.at[b], gat.at[b, pl.ds(pl.multiple_of(lev * rows, rows), rows), :], load_sem.at[b])
        for b in range(n_blocks)
    ]
    small = ((cell_hbm, cell_ref), (frac_hbm, frac_ref), (value_hbm, value_ref), (var_hbm, var_ref), (lev_hbm, lev_ref))
    small += tuple((ens_hbm.at[:, level, :], state.at[level]) for level in range(lev_rows))
    for i, (src, dst) in enumerate(small):
        loads.append(pltpu.make_async_copy(src, dst, load_sem.at[n_blocks + i]))
    for load in loads:
        load.start()

    def on_slab(k):
        p = lax.rem(slab + k, n_slab)
        return p, (p, lev)

    def on_line(k):
        return (slab, lax.rem(lev + k, n_lev))

    barrier = pltpu.get_barrier_semaphore()
    for k in range(1, n_lev):
        pl.semaphore_signal(barrier, inc=1, device_id=on_line(k), device_id_type=MESH)
    for k in range(1, n_slab):
        pl.semaphore_signal(barrier, inc=1, device_id=on_slab(k)[1], device_id_type=MESH)
    pl.semaphore_wait(barrier, n_slab + n_lev - 2)

    def hop(step, b, source, c, sem):
        spot = gat.at[
            b, pl.ds(pl.multiple_of(source * rows, rows), rows), pl.ds(pl.multiple_of(c * width, width), width)
        ]
        return pltpu.make_async_remote_copy(
            src_ref=spot, dst_ref=spot, send_sem=sem, recv_sem=line_recv.at[b, source, c],
            device_id=(slab, lev + step), device_id_type=MESH)

    ends = ((0, 1, lev < n_lev - 1), (1, -1, lev > 0))

    def send_own_first(c, carry):
        for way, step, alive in ends:
            @pl.when(alive)
            def _():
                hop(step, 0, lev, c, first_send.at[way, c]).start()
        return carry

    loads[0].wait()
    lax.fori_loop(0, chunks, send_own_first, 0)

    def send(way, step, d, b, source, c, order):
        sem = line_send.at[way, d, lax.rem(order, 2)]

        @pl.when(order >= 2)
        def _():
            hop(step, b, source, c, sem).wait_send()

        hop(step, b, source, c, sem).start()

    def forward(b, s):
        for d in range(1, n_lev):
            c = s - (d - 1) * SKEW

            @pl.when((c >= 0) & (c < chunks))
            def _():
                for way, step, alive in ends:
                    source = lev - step * d

                    @pl.when((source >= 0) & (source < n_lev))
                    def _():
                        hop(step, b, source, c, line_send.at[way, d, 0]).wait_recv()
                        if d < n_lev - 1:
                            @pl.when(alive)
                            def _():
                                send(way, step, d, b, source, c, c + b * chunks)

        for nxt in range(1, n_blocks):
            c = s + (b - nxt + 1) * steps - chunks

            @pl.when((c >= 0) & (c < chunks))
            def _():
                for way, step, alive in ends:
                    @pl.when(alive)
                    def _():
                        send(way, step, 0, nxt, lev, c, c + (nxt - 1) * chunks)

    def forwards(b, start, stop):
        def body(s, carry):
            forward(b, s)
            return carry
        lax.fori_loop(start, stop, body, 0)

    def locate(b):
        cell = jnp.broadcast_to(cell_ref[b : b + 1, :], (SUBLANES, n_obs))
        rest = cell - lev * (lev_rows * total)
        row = jnp.zeros_like(rest)
        for level in range(1, lev_rows):
            row = row + (rest >= level * total).astype(jnp.int32)
        col = rest - row * total
        following = jnp.where(col + 1 == total, 0, col + 1)
        in_band = (rest >= 0) & (rest < lev_rows * total)
        for i, where in enumerate((col, following)):
            local = where - slab * cols
            mine = in_band & (local >= 0) & (local < cols)
            local = jnp.where(mine, local, 0)
            window = row * tiles + lax.shift_right_logical(local, 7)
            window = jnp.where(mine, window, -1)
            lane = local & (LANES - 1)
            for t in range(obs_tiles):
                at = slice(t * LANES, (t + 1) * LANES)
                keys[b, i, t, 0] = window[:, at]
                keys[b, i, t, 1] = lane[:, at]


    def gather(b, c):
        for i in range(2):
            for t in range(obs_tiles):
                at = slice(t * LANES, (t + 1) * LANES)
                now = acc[i, :, at]
                window = keys[b, i, t, 0]
                lane = jnp.concatenate([keys[b, i, t, 1]] * (members // SUBLANES), axis=0)
                for level in range(lev_rows):
                    for w in range(wide):
                        tile = c * wide + w
                        hit = (window == level * tiles + tile).astype(jnp.int32)
                        hit = jnp.concatenate([hit] * (members // SUBLANES), axis=0)
                        held = state[level, :, pl.ds(pl.multiple_of(tile * LANES, LANES), LANES)]
                        got = jnp.take_along_axis(held, lane, axis=1, mode="promise_in_bounds")
                        now = jnp.where(hit > 0, got, now)
                acc[i, :, at] = now

    def finish_pick(b):
        frac = frac_ref[b : b + 1, :]
        value = acc[0] * (1.0 - frac) + acc[1] * frac
        pad = jnp.zeros((LANES - members, LANES), F32)
        for t in range(obs_tiles):
            at = slice(t * LANES, (t + 1) * LANES)
            part[b, at, :] = jnp.concatenate([value[:, at], pad], axis=0).T

    def pick_first(c, carry):
        gather(0, c)
        return carry

    def scatter(b, k):
        p, where = on_slab(k)
        return pltpu.make_async_remote_copy(
            src_ref=part.at[b, pl.ds(pl.multiple_of(p * slots, slots), slots), :], dst_ref=landed.at[b, k],
            send_sem=scat_send.at[b, k], recv_sem=scat_recv.at[b, k], device_id=where, device_id_type=MESH)

    def along(b, k):
        return pltpu.make_async_remote_copy(
            src_ref=zown.at[b], dst_ref=zland.at[b, k],
            send_sem=z_send.at[b, k], recv_sem=z_recv.at[b, k], device_id=on_line(k), device_id_type=MESH)

    def cast(b, k):
        return pltpu.make_async_remote_copy(
            src_ref=own.at[b], dst_ref=prior.at[b, slab],
            send_sem=cast_send.at[b, k], recv_sem=cast_recv.at[b, k], device_id=on_slab(k)[1], device_id_type=MESH)

    def exchange(b, fills):
        for k in range(1, n_slab):
            scatter(b, k).start()
        forwards(b, 0, fills[0])
        value = part[b, pl.ds(pl.multiple_of(slab * slots, slots), slots), :]
        for k in range(1, n_slab):
            scatter(b, k).wait_recv()
        for k in range(1, n_slab):
            value = value + landed[b, k]
        zown[b] = value
        for k in range(1, n_lev):
            along(b, k).start()
        forwards(b, fills[0], fills[0] + fills[1])
        for k in range(1, n_lev):
            along(b, k).wait_recv()
        for k in range(1, n_lev):
            value = value + zland[b, k]
        own[b] = value
        for k in range(1, n_slab):
            cast(b, k).start()
        prior[b, slab] = value
        forwards(b, fills[0] + fills[1], sum(fills))
        for k in range(1, n_slab):
            cast(b, k).wait_recv()

    def statistics(b):
        def column(ref):
            return jnp.broadcast_to(ref[b : b + 1, :], (SUBLANES, n_obs)).T[:, :1]

        value, var = column(value_ref), column(var_ref)
        now = prior[b].reshape(n_obs, LANES)
        live = lax.broadcasted_iota(jnp.int32, now.shape, 1) < members
        mean = jnp.sum(jnp.where(live, now, 0.0), axis=1, keepdims=True) / members
        deviation = jnp.where(live, now - mean, 0.0)
        spread = jnp.sum(deviation * deviation, axis=1, keepdims=True) / (members - 1.0)
        whole = spread + var
        shrink = 1.0 / (1.0 + jnp.sqrt(var / whole))
        gain = ((value - mean) - deviation * shrink) / (whole * (members - 1.0))
        dev_s[...] = deviation.astype(BF16)
        gain_s[...] = gain.T.astype(BF16)
        mean_ref[b : b + 1, :] = jnp.broadcast_to(mean, (n_obs, LANES)).T[:1, :]

    def spread_levels(b):
        for level in range(lev_rows):
            lev_s[level] = jnp.broadcast_to(lev_ref[b, level : level + 1, :], (LANES, n_obs)).T

    def update(b, c):
        at = pl.ds(pl.multiple_of(c * width, width), width)
        dev = dev_s[:, :members]
        gain = gain_s[:members, :]
        loc = gat[b, :, at].astype(F32)
        levels = range(lev_rows)
        now = [state[level, :, at] for level in levels]
        centred = [(x - jnp.sum(x, axis=0, keepdims=True) / members).astype(BF16) for x in now]
        cross = [jnp.dot(dev, x, preferred_element_type=F32) for x in centred]
        height = [jnp.concatenate([lev_s[level]] * wide, axis=1) for level in levels]
        mixed = [((height[level] * loc) * cross[level]).astype(BF16) for level in levels]
        new = [now[level] + jnp.dot(gain, mixed[level], preferred_element_type=F32) for level in levels]
        for level in levels:
            state[level, :, at] = new[level]
        if b + 1 < n_blocks:
            gather(b + 1, c)

    acc[...] = jnp.zeros_like(acc)
    for load in loads[1:]:
        load.wait()
    for b in range(n_blocks):
        locate(b)
    lax.fori_loop(0, chunks, pick_first, 0)
    finish_pick(0)
    for b in range(n_blocks):
        fills = STEPS_FIRST if b == 0 else STEPS_LATER
        spread_levels(b)
        exchange(b, fills)
        statistics(b)
        if b + 1 < n_blocks:
            acc[...] = jnp.zeros_like(acc)
        done = sum(fills)
        early = max(done - lag, 0)

        def double(s, carry):
            forward(b, s)
            update(b, 2 * (s - done))
            update(b, 2 * (s - done) + 1)
            return carry

        def single(s, carry):
            forward(b, s)
            update(b, s - lag)
            return carry

        forwards(b, done, lag)
        lax.fori_loop(lag + early, lag + 2 * early, double, 0)
        lax.fori_loop(lag + 2 * early, steps, single, 0)
        if b + 1 < n_blocks:
            finish_pick(b + 1)

    def drain_first(c, carry):
        for way, step, alive in ends:
            @pl.when(alive)
            def _():
                hop(step, 0, lev, c, first_send.at[way, c]).wait_send()
        return carry

    lax.fori_loop(0, chunks, drain_first, 0)
    for way, step, alive in ends:
        @pl.when(alive)
        def _():
            for d in range(n_lev - 1):
                if d == 0 and n_blocks == 1:
                    continue
                source = lev - step * d

                @pl.when((source >= 0) & (source < n_lev))
                def _():
                    for slot in range(2):
                        hop(step, 0, source, 0, line_send.at[way, d, slot]).wait_send()
    for b in range(n_blocks):
        for k in range(1, n_slab):
            scatter(b, k).wait_send()
            cast(b, k).wait_send()
        for k in range(1, n_lev):
            along(b, k).wait_send()


def analyse(n_slab, n_lev, ensemble, cells, values, variances, fracs, locs, heights):
    members, lev_rows, cols = ensemble.shape
    n_blocks, n_obs = cells.shape
    rows = locs.shape[1]
    width = next(t * LANES for t in (2, 1) if cols % (t * LANES) == 0)
    chunks = cols // width
    slots = n_obs // n_slab
    vmem = pl.BlockSpec(memory_space=pltpu.VMEM)
    hbm = pl.BlockSpec(memory_space=pltpu.HBM)
    dma = pltpu.SemaphoreType.DMA
    return pl.pallas_call(
        functools.partial(kernel, n_slab, n_lev),
        out_shape=[
            pltpu.VMEM((lev_rows, members, cols), F32),
            pltpu.VMEM(values.shape, F32),
        ],
        in_specs=[hbm] * 7,
        out_specs=[vmem, vmem],
        scratch_shapes=[
            pltpu.VMEM(cells.shape, jnp.int32),
            pltpu.VMEM(fracs.shape, F32),
            pltpu.VMEM(values.shape, F32),
            pltpu.VMEM(variances.shape, F32),
            pltpu.VMEM(heights.shape, F32),
            pltpu.VMEM((n_blocks, n_obs, cols), BF16),
            pltpu.VMEM((n_blocks, 2, n_obs // LANES, 2, SUBLANES, LANES), jnp.int32),
            pltpu.VMEM((2, members, n_obs), F32),
            pltpu.VMEM((n_blocks, n_obs, LANES), F32),
            pltpu.VMEM((n_blocks, n_slab, slots, LANES), F32),
            pltpu.VMEM((n_blocks, slots, LANES), F32),
            pltpu.VMEM((n_blocks, n_lev, slots, LANES), F32),
            pltpu.VMEM((n_blocks, slots, LANES), F32),
            pltpu.VMEM((n_blocks, n_slab, slots, LANES), F32),
            pltpu.VMEM((n_obs, LANES), BF16),
            pltpu.VMEM((LANES, n_obs), BF16),
            pltpu.VMEM((lev_rows, n_obs, LANES), F32),
            dma((n_blocks + 5 + lev_rows,)),
            dma((n_blocks, n_lev, chunks)),
            dma((2, chunks)),
            dma((2, n_lev, 2)),
            dma((n_blocks, n_slab)),
            dma((n_blocks, n_slab)),
            dma((n_blocks, n_lev)),
            dma((n_blocks, n_lev)),
            dma((n_blocks, n_slab)),
            dma((n_blocks, n_slab)),
        ],
        compiler_params=pltpu.CompilerParams(collective_id=0, has_side_effects=True, vmem_limit_bytes=28 << 20),
        name="analyse",
    )(*(pltpu.with_memory_space_constraint(x, pltpu.HBM) for x in (cells, fracs, values, variances, heights, ensemble, locs)))


def hand_over_kernel(state, means, out_ref, mean_ref, sem):
    lev_rows = state.shape[0]
    copies = [pltpu.make_async_copy(state.at[level], out_ref.at[:, level, :], sem.at[level]) for level in range(lev_rows)]
    copies.append(pltpu.make_async_copy(means, mean_ref, sem.at[lev_rows]))
    for copy in copies:
        copy.start()
    for copy in copies:
        copy.wait()


def hand_over(state, means):
    lev_rows, members, cols = state.shape
    vmem = pl.BlockSpec(memory_space=pltpu.VMEM)
    hbm = pl.BlockSpec(memory_space=pltpu.HBM)
    return pl.pallas_call(
        hand_over_kernel,
        out_shape=[pltpu.HBM((members, lev_rows, cols), F32), pltpu.HBM(means.shape, F32)],
        in_specs=[vmem, vmem],
        out_specs=[hbm, hbm],
        scratch_shapes=[pltpu.SemaphoreType.DMA((lev_rows + 1,))],
        compiler_params=pltpu.CompilerParams(vmem_limit_bytes=8 << 20),
        name="hand_over",
    )(*(pltpu.with_memory_space_constraint(x, pltpu.VMEM) for x in (state, means)))


def solution(mesh):
    n_slab, n_lev = mesh.shape["slab"], mesh.shape["lev"]

    def on_device(ensemble, obs_cell, obs_value, obs_var, obs_frac, loc_column, loc_level):
        heights = loc_level.transpose(0, 2, 1)
        state, means = analyse(n_slab, n_lev, ensemble, obs_cell, obs_value, obs_var, obs_frac, loc_column, heights)
        return tuple(hand_over(state, means))

    in_specs = (
        P(None, "lev", "slab"), P(), P(), P(), P(),
        P(None, "lev", "slab"), P(None, None, "lev"),
    )
    return jax.shard_map(
        on_device, mesh=mesh, in_specs=in_specs,
        out_specs=(P(None, "lev", "slab"), P()), check_vma=False,
    )
```

```python
import functools

import jax
import jax.numpy as jnp
from jax import lax
from jax.experimental import pallas as pl
from jax.experimental.pallas import tpu as pltpu
from jax.sharding import PartitionSpec as P

MESH = pl.DeviceIdType.MESH
LANES = 128
SUBLANES = 8
F32 = jnp.float32
BF16 = jnp.bfloat16
SKEW = 3
STEPS_FIRST = (3, 3, 2)
STEPS_LATER = (4, 3, 2)


def kernel(
    n_slab, n_lev, cell_hbm, frac_hbm, value_hbm, var_hbm, lev_hbm, ens_hbm, loc_hbm, state, mean_ref,
    cell_ref, frac_ref, value_ref, var_ref, lev_ref, gat, keys, acc, part, landed, zown, zland, own, prior, dev_s, gain_s, lev_s,
    load_sem, line_recv, own_send, line_send, scat_send, scat_recv, z_send, z_recv, cast_send, cast_recv,
):
    lev_rows, members, cols = state.shape
    n_blocks, n_obs = cell_hbm.shape
    rows = loc_hbm.shape[1]
    tiles = cols // LANES
    chunks = line_recv.shape[2]
    width = cols // chunks
    wide = width // LANES
    total = cols * n_slab
    slots = own.shape[1]
    lag = SKEW * (n_lev - 2)
    steps = chunks + lag
    obs_tiles = n_obs // LANES
    slab, lev = lax.axis_index("slab"), lax.axis_index("lev")

    mine = pl.ds(pl.multiple_of(lev * rows, rows), rows)
    small = ((cell_hbm, cell_ref), (frac_hbm, frac_ref), (value_hbm, value_ref), (var_hbm, var_ref), (lev_hbm, lev_ref))
    loads = [(loc_hbm.at[b], gat.at[b, mine, :]) for b in range(n_blocks)] + list(small)
    loads = [pltpu.make_async_copy(src, dst, load_sem.at[i]) for i, (src, dst) in enumerate(loads)]
    state_sem = load_sem.at[len(loads)]
    for load in loads[:n_blocks]:
        load.start()
    for level in range(lev_rows):
        pltpu.make_async_copy(ens_hbm.at[:, level, :], state.at[level], state_sem).start()
    for load in loads[n_blocks:]:
        load.start()

    def on_slab(k):
        p = lax.rem(slab + k, n_slab)
        return p, (p, lev)

    def on_line(k):
        return (slab, lax.rem(lev + k, n_lev))

    barrier = pltpu.get_barrier_semaphore()
    for k in range(1, n_lev):
        pl.semaphore_signal(barrier, inc=1, device_id=on_line(k), device_id_type=MESH)
    for k in range(1, n_slab):
        pl.semaphore_signal(barrier, inc=1, device_id=on_slab(k)[1], device_id_type=MESH)
    pl.semaphore_wait(barrier, n_slab + n_lev - 2)

    def hop(step, b, source, c, sem):
        spot = gat.at[
            b, pl.ds(pl.multiple_of(source * rows, rows), rows), pl.ds(pl.multiple_of(c * width, width), width)
        ]
        there = lev + step
        slot = source - (source > there).astype(jnp.int32)
        return pltpu.make_async_remote_copy(
            src_ref=spot, dst_ref=spot, send_sem=sem, recv_sem=line_recv.at[b, slot, c],
            device_id=(slab, there), device_id_type=MESH)

    def landing(b, source, c, sem):
        slot = source - (source > lev).astype(jnp.int32)
        spot = gat.at[
            b, pl.ds(pl.multiple_of(source * rows, rows), rows), pl.ds(pl.multiple_of(c * width, width), width)
        ]
        return pltpu.make_async_remote_copy(
            src_ref=spot, dst_ref=spot, send_sem=sem, recv_sem=line_recv.at[b, slot, c],
            device_id=(slab, lev), device_id_type=MESH)

    ends = ((0, 1, lev < n_lev - 1), (1, -1, lev > 0))

    def send_own(b):
        def body(c, carry):
            for way, step, alive in ends:
                @pl.when(alive)
                def _():
                    hop(step, b, lev, c, own_send.at[b, way]).start()
            return carry
        lax.fori_loop(0, chunks, body, 0)

    loads[0].wait()
    send_own(0)

    def send(way, step, d, b, source, c, order):
        sem = line_send.at[way, d - 1, lax.rem(order, 2)]

        @pl.when(order >= 2)
        def _():
            hop(step, b, source, c, sem).wait_send()

        hop(step, b, source, c, sem).start()

    def forward(b, s):
        for d in range(1, n_lev):
            c = s - (d - 1) * SKEW

            @pl.when((c >= 0) & (c < chunks))
            def _():
                for way, step, alive in ends:
                    source = lev - step * d

                    @pl.when((source >= 0) & (source < n_lev))
                    def _():
                        landing(b, source, c, line_send.at[way, 0, 0]).wait_recv()
                        if d < n_lev - 1:
                            @pl.when(alive)
                            def _():
                                send(way, step, d, b, source, c, c + b * chunks)

    def forwards(b, start, stop):
        def body(s, carry):
            forward(b, s)
            return carry
        lax.fori_loop(start, stop, body, 0)

    def locate(b):
        cell = jnp.broadcast_to(cell_ref[b : b + 1, :], (SUBLANES, n_obs))
        rest = cell - lev * (lev_rows * total)
        row = jnp.zeros_like(rest)
        for level in range(1, lev_rows):
            row = row + (rest >= level * total).astype(jnp.int32)
        col = rest - row * total
        following = jnp.where(col + 1 == total, 0, col + 1)
        in_band = (rest >= 0) & (rest < lev_rows * total)
        for i, where in enumerate((col, following)):
            local = where - slab * cols
            mine = in_band & (local >= 0) & (local < cols)
            local = jnp.where(mine, local, 0)
            window = row * tiles + lax.shift_right_logical(local, 7)
            window = jnp.where(mine, window, -1)
            lane = local & (LANES - 1)
            for t in range(obs_tiles):
                at = slice(t * LANES, (t + 1) * LANES)
                keys[b, i, t, 0] = window[:, at]
                keys[b, i, t, 1] = lane[:, at]


    def gather(b, c):
        for i in range(2):
            for t in range(obs_tiles):
                at = slice(t * LANES, (t + 1) * LANES)
                now = acc[i, :, at]
                window = keys[b, i, t, 0]
                lane = jnp.concatenate([keys[b, i, t, 1]] * (members // SUBLANES), axis=0)
                for level in range(lev_rows):
                    for w in range(wide):
                        tile = c * wide + w
                        hit = (window == level * tiles + tile).astype(jnp.int32)
                        hit = jnp.concatenate([hit] * (members // SUBLANES), axis=0)
                        held = state[level, :, pl.ds(pl.multiple_of(tile * LANES, LANES), LANES)]
                        got = jnp.take_along_axis(held, lane, axis=1, mode="promise_in_bounds")
                        now = jnp.where(hit > 0, got, now)
                acc[i, :, at] = now

    def finish_pick(b):
        frac = frac_ref[b : b + 1, :]
        value = acc[0] * (1.0 - frac) + acc[1] * frac
        for t in range(obs_tiles):
            part[b, t * members : (t + 1) * members, :] = value[:, t * LANES : (t + 1) * LANES]

    def pick_first(c, carry):
        gather(0, c)
        return carry

    def scatter(b, k):
        p, where = on_slab(k)
        return pltpu.make_async_remote_copy(
            src_ref=part.at[b, pl.ds(pl.multiple_of(p * slots, slots), slots), :], dst_ref=landed.at[b, k - 1],
            send_sem=scat_send.at[b], recv_sem=scat_recv.at[b], device_id=where, device_id_type=MESH)

    def scattered(b):
        return pltpu.make_async_remote_copy(
            src_ref=landed.at[b], dst_ref=landed.at[b],
            send_sem=scat_send.at[b], recv_sem=scat_recv.at[b], device_id=on_slab(1)[1], device_id_type=MESH)

    def collected(b):
        some = prior.at[b, pl.ds(0, n_slab - 1)]
        return pltpu.make_async_remote_copy(
            src_ref=some, dst_ref=some,
            send_sem=cast_send.at[b], recv_sem=cast_recv.at[b], device_id=on_slab(1)[1], device_id_type=MESH)

    def along(b, k):
        return pltpu.make_async_remote_copy(
            src_ref=zown.at[b], dst_ref=zland.at[b, k],
            send_sem=z_send.at[b, k], recv_sem=z_recv.at[b, k], device_id=on_line(k), device_id_type=MESH)

    def cast(b, k):
        return pltpu.make_async_remote_copy(
            src_ref=own.at[b], dst_ref=prior.at[b, slab],
            send_sem=cast_send.at[b], recv_sem=cast_recv.at[b], device_id=on_slab(k)[1], device_id_type=MESH)

    def exchange(b, fills):
        for k in range(1, n_slab):
            scatter(b, k).start()
        forwards(b, 0, fills[0])
        value = part[b, pl.ds(pl.multiple_of(slab * slots, slots), slots), :]
        scattered(b).wait_recv()
        for k in range(n_slab - 1):
            value = value + landed[b, k]
        zown[b] = value
        for k in range(1, n_lev):
            along(b, k).start()
        forwards(b, fills[0], fills[0] + fills[1])
        for k in range(1, n_lev):
            along(b, k).wait_recv()
        for k in range(1, n_lev):
            value = value + zland[b, k]
        own[b] = value
        for k in range(1, n_slab):
            cast(b, k).start()
        prior[b, slab] = value
        forwards(b, fills[0] + fills[1], sum(fills))
        collected(b).wait_recv()

    def statistics(b):
        now = prior[b].reshape(n_slab * slots, LANES)
        now = jnp.concatenate([now[t * members : (t + 1) * members] for t in range(obs_tiles)], axis=1)
        value, var = value_ref[b : b + 1, :], var_ref[b : b + 1, :]
        mean = jnp.sum(now, axis=0, keepdims=True) / members
        deviation = now - mean
        spread = jnp.sum(deviation * deviation, axis=0, keepdims=True) / (members - 1.0)
        whole = spread + var
        shrink = 1.0 / (1.0 + jnp.sqrt(var / whole))
        gain = ((value - mean) - deviation * shrink) / (whole * (members - 1.0))
        pad = jnp.zeros((LANES - members, n_obs), F32)
        dev_s[...] = jnp.concatenate([deviation, pad], axis=0).T.astype(BF16)
        gain_s[...] = gain.astype(BF16)
        mean_ref[b : b + 1, :] = mean

    def spread_levels(b):
        for level in range(lev_rows):
            lev_s[level] = jnp.broadcast_to(lev_ref[b, level : level + 1, :], (LANES, n_obs)).T

    def update(b, c):
        at = pl.ds(pl.multiple_of(c * width, width), width)
        dev = dev_s[:, :members]
        gain = gain_s[...]
        loc = gat[b, :, at].astype(F32)
        levels = range(lev_rows)
        now = [state[level, :, at] for level in levels]
        centred = [(x - jnp.sum(x, axis=0, keepdims=True) / members).astype(BF16) for x in now]
        cross = [jnp.dot(dev, x, preferred_element_type=F32) for x in centred]
        height = [jnp.concatenate([lev_s[level]] * wide, axis=1) for level in levels]
        mixed = [((height[level] * loc) * cross[level]).astype(BF16) for level in levels]
        new = [now[level] + jnp.dot(gain, mixed[level], preferred_element_type=F32) for level in levels]
        for level in levels:
            state[level, :, at] = new[level]
    acc[...] = jnp.zeros_like(acc)
    part[...] = jnp.zeros_like(part)
    for load in loads[1:]:
        load.wait()
    pltpu.make_async_copy(state, state, state_sem).wait()
    for b in range(n_blocks):
        locate(b)
    lax.fori_loop(0, chunks, pick_first, 0)
    finish_pick(0)
    for b in range(n_blocks):
        fills = STEPS_FIRST if b == 0 else STEPS_LATER
        spread_levels(b)
        exchange(b, fills)
        statistics(b)
        if b + 1 < n_blocks:
            acc[...] = jnp.zeros_like(acc)
        done = sum(fills)
        early = max(done - lag, 0)

        def advance(c):
            if b + 1 < n_blocks:
                gather(b + 1, c - 1)
            update(b, c)

        def plain(c, carry):
            advance(c)
            return carry

        def double(s, carry):
            forward(b, s)
            update(b, 2 * (s - done))
            update(b, 2 * (s - done) + 1)
            return carry

        def single(s, carry):
            forward(b, s)
            advance(s - lag)
            return carry

        if b + 1 < n_blocks:
            sent = steps - SKEW

            forwards(b, done, lag + 1)
            base = max(done, lag + 1)
            forward(b, base)
            update(b, 0)

            def between(s, carry):
                forward(b, s)
                advance(s - base)
                return carry

            lax.fori_loop(base + 1, sent, between, 0)
            send_own(b + 1)
            lax.fori_loop(sent - base, sent - lag, plain, 0)
            lax.fori_loop(sent, steps, single, 0)
            gather(b + 1, chunks - 1)
        else:
            forwards(b, done, lag)
            lax.fori_loop(lag + early, lag + 2 * early, double, 0)
            lax.fori_loop(lag + 2 * early, steps, single, 0)
        if b + 1 < n_blocks:
            finish_pick(b + 1)

    for way, step, alive in ends:
        @pl.when(alive)
        def _():
            for b in range(n_blocks):
                whole = gat.at[b, mine, :]
                pltpu.make_async_remote_copy(
                    src_ref=whole, dst_ref=whole, send_sem=own_send.at[b, way], recv_sem=line_recv.at[0, 0, 0],
                    device_id=(slab, lev + step), device_id_type=MESH).wait_send()
            for d in range(1, n_lev - 1):
                source = lev - step * d

                @pl.when((source >= 0) & (source < n_lev))
                def _():
                    for slot in range(2):
                        hop(step, 0, source, 0, line_send.at[way, d - 1, slot]).wait_send()
    for b in range(n_blocks):
        scattered(b).wait_send()
        collected(b).wait_send()
        for k in range(1, n_lev):
            along(b, k).wait_send()


def analyse(n_slab, n_lev, ensemble, cells, values, variances, fracs, locs, heights):
    members, lev_rows, cols = ensemble.shape
    n_blocks, n_obs = cells.shape
    rows = locs.shape[1]
    width = next(t * LANES for t in (2, 1) if cols % (t * LANES) == 0)
    chunks = cols // width
    packed = members * (n_obs // LANES)
    slots = pl.cdiv(packed, n_slab * SUBLANES) * SUBLANES
    vmem = pl.BlockSpec(memory_space=pltpu.VMEM)
    hbm = pl.BlockSpec(memory_space=pltpu.HBM)
    dma = pltpu.SemaphoreType.DMA
    return pl.pallas_call(
        functools.partial(kernel, n_slab, n_lev),
        out_shape=[
            pltpu.VMEM((lev_rows, members, cols), F32),
            pltpu.VMEM(values.shape, F32),
        ],
        in_specs=[hbm] * 7,
        out_specs=[vmem, vmem],
        scratch_shapes=[
            pltpu.VMEM(cells.shape, jnp.int32),
            pltpu.VMEM(fracs.shape, F32),
            pltpu.VMEM(values.shape, F32),
            pltpu.VMEM(variances.shape, F32),
            pltpu.VMEM(heights.shape, F32),
            pltpu.VMEM((n_blocks, n_obs, cols), BF16),
            pltpu.VMEM((n_blocks, 2, n_obs // LANES, 2, SUBLANES, LANES), jnp.int32),
            pltpu.VMEM((2, members, n_obs), F32),
            pltpu.VMEM((n_blocks, n_slab * slots, LANES), F32),
            pltpu.VMEM((n_blocks, n_slab - 1, slots, LANES), F32),
            pltpu.VMEM((n_blocks, slots, LANES), F32),
            pltpu.VMEM((n_blocks, n_lev, slots, LANES), F32),
            pltpu.VMEM((n_blocks, slots, LANES), F32),
            pltpu.VMEM((n_blocks, n_slab, slots, LANES), F32),
            pltpu.VMEM((n_obs, LANES), BF16),
            pltpu.VMEM((members, n_obs), BF16),
            pltpu.VMEM((lev_rows, n_obs, LANES), F32),
            dma((n_blocks + 6,)),
            dma((n_blocks, n_lev - 1, chunks)),
            dma((n_blocks, 2)),
            dma((2, n_lev - 2, 2)),
            dma((n_blocks,)),
            dma((n_blocks,)),
            dma((n_blocks, n_lev)),
            dma((n_blocks, n_lev)),
            dma((n_blocks,)),
            dma((n_blocks,)),
        ],
        compiler_params=pltpu.CompilerParams(collective_id=0, has_side_effects=True, vmem_limit_bytes=28 << 20),
        name="analyse",
    )(*(pltpu.with_memory_space_constraint(x, pltpu.HBM) for x in (cells, fracs, values, variances, heights, ensemble, locs)))


def hand_over_kernel(state, means, out_ref, mean_ref, sem):
    lev_rows = state.shape[0]
    copies = [pltpu.make_async_copy(state.at[level], out_ref.at[:, level, :], sem.at[level]) for level in range(lev_rows)]
    copies.append(pltpu.make_async_copy(means, mean_ref, sem.at[lev_rows]))
    for copy in copies:
        copy.start()
    for copy in copies:
        copy.wait()


def hand_over(state, means):
    lev_rows, members, cols = state.shape
    vmem = pl.BlockSpec(memory_space=pltpu.VMEM)
    hbm = pl.BlockSpec(memory_space=pltpu.HBM)
    return pl.pallas_call(
        hand_over_kernel,
        out_shape=[pltpu.HBM((members, lev_rows, cols), F32), pltpu.HBM(means.shape, F32)],
        in_specs=[vmem, vmem],
        out_specs=[hbm, hbm],
        scratch_shapes=[pltpu.SemaphoreType.DMA((lev_rows + 1,))],
        compiler_params=pltpu.CompilerParams(vmem_limit_bytes=8 << 20),
        name="hand_over",
    )(*(pltpu.with_memory_space_constraint(x, pltpu.VMEM) for x in (state, means)))


def solution(mesh):
    n_slab, n_lev = mesh.shape["slab"], mesh.shape["lev"]

    def on_device(ensemble, obs_cell, obs_value, obs_var, obs_frac, loc_column, loc_level):
        heights = loc_level.transpose(0, 2, 1)
        state, means = analyse(n_slab, n_lev, ensemble, obs_cell, obs_value, obs_var, obs_frac, loc_column, heights)
        return tuple(hand_over(state, means))

    in_specs = (
        P(None, "lev", "slab"), P(), P(), P(), P(),
        P(None, "lev", "slab"), P(None, None, "lev"),
    )
    return jax.shard_map(
        on_device, mesh=mesh, in_specs=in_specs,
        out_specs=(P(None, "lev", "slab"), P()), check_vma=False,
    )
```

```python
import functools

import jax
import jax.numpy as jnp
from jax import lax
from jax.experimental import pallas as pl
from jax.experimental.pallas import tpu as pltpu
from jax.sharding import PartitionSpec as P

MESH = pl.DeviceIdType.MESH
LANES = 128
SUBLANES = 8
F32 = jnp.float32
BF16 = jnp.bfloat16
SKEW = 3
STEPS_FIRST = (3, 3, 2)
STEPS_LATER = (3, 3, 2)


def kernel(
    n_slab, n_lev, cell_hbm, frac_hbm, value_hbm, var_hbm, lev_hbm, ens_hbm, loc_hbm, state, mean_ref,
    cell_ref, frac_ref, value_ref, var_ref, lev_ref, gat, keys, acc, part, landed, zown, zland, own, prior, dev_s, gain_s, lev_s,
    load_sem, line_recv, own_send, line_send, scat_send, scat_recv, z_send, z_recv, cast_send, cast_recv,
):
    lev_rows, members, cols = state.shape
    n_blocks, n_obs = cell_hbm.shape
    rows = loc_hbm.shape[1]
    tiles = cols // LANES
    chunks = line_recv.shape[2]
    width = cols // chunks
    wide = width // LANES
    total = cols * n_slab
    slots = own.shape[1]
    lag = SKEW * (n_lev - 2)
    steps = chunks + lag
    obs_tiles = n_obs // LANES
    slab, lev = lax.axis_index("slab"), lax.axis_index("lev")

    mine = pl.ds(pl.multiple_of(lev * rows, rows), rows)
    small = ((cell_hbm, cell_ref), (frac_hbm, frac_ref), (value_hbm, value_ref), (var_hbm, var_ref), (lev_hbm, lev_ref))
    loads = [(loc_hbm.at[b], gat.at[b, mine, :]) for b in range(n_blocks)] + list(small)
    loads = [pltpu.make_async_copy(src, dst, load_sem.at[i]) for i, (src, dst) in enumerate(loads)]
    state_sem = load_sem.at[len(loads)]
    for load in loads[:n_blocks]:
        load.start()
    for level in range(lev_rows):
        pltpu.make_async_copy(ens_hbm.at[:, level, :], state.at[level], state_sem).start()
    for load in loads[n_blocks:]:
        load.start()

    def on_slab(k):
        p = lax.rem(slab + k, n_slab)
        return p, (p, lev)

    def on_line(k):
        return (slab, lax.rem(lev + k, n_lev))

    barrier = pltpu.get_barrier_semaphore()
    for k in range(1, n_lev):
        pl.semaphore_signal(barrier, inc=1, device_id=on_line(k), device_id_type=MESH)
    for k in range(1, n_slab):
        pl.semaphore_signal(barrier, inc=1, device_id=on_slab(k)[1], device_id_type=MESH)
    pl.semaphore_wait(barrier, n_slab + n_lev - 2)

    def hop(step, b, source, c, sem):
        spot = gat.at[
            b, pl.ds(pl.multiple_of(source * rows, rows), rows), pl.ds(pl.multiple_of(c * width, width), width)
        ]
        there = lev + step
        slot = source - (source > there).astype(jnp.int32)
        return pltpu.make_async_remote_copy(
            src_ref=spot, dst_ref=spot, send_sem=sem, recv_sem=line_recv.at[b, slot, c],
            device_id=(slab, there), device_id_type=MESH)

    def landing(b, source, c, sem):
        slot = source - (source > lev).astype(jnp.int32)
        spot = gat.at[
            b, pl.ds(pl.multiple_of(source * rows, rows), rows), pl.ds(pl.multiple_of(c * width, width), width)
        ]
        return pltpu.make_async_remote_copy(
            src_ref=spot, dst_ref=spot, send_sem=sem, recv_sem=line_recv.at[b, slot, c],
            device_id=(slab, lev), device_id_type=MESH)

    ends = ((0, 1, lev < n_lev - 1), (1, -1, lev > 0))

    def send_own(b):
        def body(c, carry):
            for way, step, alive in ends:
                @pl.when(alive)
                def _():
                    hop(step, b, lev, c, own_send.at[b, way]).start()
            return carry
        lax.fori_loop(0, chunks, body, 0)

    loads[0].wait()
    send_own(0)

    def send(way, step, d, b, source, c, order):
        sem = line_send.at[way, d - 1, lax.rem(order, 2)]

        @pl.when(order >= 2)
        def _():
            hop(step, b, source, c, sem).wait_send()

        hop(step, b, source, c, sem).start()

    def forward(b, s):
        for d in range(1, n_lev):
            c = s - (d - 1) * SKEW

            @pl.when((c >= 0) & (c < chunks))
            def _():
                for way, step, alive in ends:
                    source = lev - step * d

                    @pl.when((source >= 0) & (source < n_lev))
                    def _():
                        landing(b, source, c, line_send.at[way, 0, 0]).wait_recv()
                        if d < n_lev - 1:
                            @pl.when(alive)
                            def _():
                                send(way, step, d, b, source, c, c + b * chunks)

    def forwards(b, start, stop):
        def body(s, carry):
            forward(b, s)
            return carry
        lax.fori_loop(start, stop, body, 0)

    def locate(b):
        cell = jnp.broadcast_to(cell_ref[b : b + 1, :], (SUBLANES, n_obs))
        rest = cell - lev * (lev_rows * total)
        row = jnp.zeros_like(rest)
        for level in range(1, lev_rows):
            row = row + (rest >= level * total).astype(jnp.int32)
        col = rest - row * total
        following = jnp.where(col + 1 == total, 0, col + 1)
        in_band = (rest >= 0) & (rest < lev_rows * total)
        for i, where in enumerate((col, following)):
            local = where - slab * cols
            mine = in_band & (local >= 0) & (local < cols)
            local = jnp.where(mine, local, 0)
            window = row * tiles + lax.shift_right_logical(local, 7)
            window = jnp.where(mine, window, -1)
            lane = local & (LANES - 1)
            for t in range(obs_tiles):
                at = slice(t * LANES, (t + 1) * LANES)
                keys[b, i, t, 0] = window[:, at]
                keys[b, i, t, 1] = lane[:, at]


    def gather(b, c):
        for i in range(2):
            for t in range(obs_tiles):
                at = slice(t * LANES, (t + 1) * LANES)
                now = acc[i, :, at]
                window = keys[b, i, t, 0]
                lane = jnp.concatenate([keys[b, i, t, 1]] * (members // SUBLANES), axis=0)
                for level in range(lev_rows):
                    for w in range(wide):
                        tile = c * wide + w
                        hit = (window == level * tiles + tile).astype(jnp.int32)
                        hit = jnp.concatenate([hit] * (members // SUBLANES), axis=0)
                        held = state[level, :, pl.ds(pl.multiple_of(tile * LANES, LANES), LANES)]
                        got = jnp.take_along_axis(held, lane, axis=1, mode="promise_in_bounds")
                        now = jnp.where(hit > 0, got, now)
                acc[i, :, at] = now

    def finish_pick(b):
        frac = frac_ref[b : b + 1, :]
        value = acc[0] * (1.0 - frac) + acc[1] * frac
        for t in range(obs_tiles):
            part[b, t * members : (t + 1) * members, :] = value[:, t * LANES : (t + 1) * LANES]

    def pick_first(c, carry):
        gather(0, c)
        return carry

    def scatter(b, k):
        p, where = on_slab(k)
        return pltpu.make_async_remote_copy(
            src_ref=part.at[b, pl.ds(pl.multiple_of(p * slots, slots), slots), :], dst_ref=landed.at[b, k - 1],
            send_sem=scat_send.at[b], recv_sem=scat_recv.at[b], device_id=where, device_id_type=MESH)

    def scattered(b):
        return pltpu.make_async_remote_copy(
            src_ref=landed.at[b], dst_ref=landed.at[b],
            send_sem=scat_send.at[b], recv_sem=scat_recv.at[b], device_id=on_slab(1)[1], device_id_type=MESH)

    def collected(b):
        some = prior.at[b, pl.ds(0, n_slab - 1)]
        return pltpu.make_async_remote_copy(
            src_ref=some, dst_ref=some,
            send_sem=cast_send.at[b], recv_sem=cast_recv.at[b], device_id=on_slab(1)[1], device_id_type=MESH)

    def along(b, k):
        return pltpu.make_async_remote_copy(
            src_ref=zown.at[b], dst_ref=zland.at[b, k],
            send_sem=z_send.at[b, k], recv_sem=z_recv.at[b, k], device_id=on_line(k), device_id_type=MESH)

    def cast(b, k):
        return pltpu.make_async_remote_copy(
            src_ref=own.at[b], dst_ref=prior.at[b, slab],
            send_sem=cast_send.at[b], recv_sem=cast_recv.at[b], device_id=on_slab(k)[1], device_id_type=MESH)

    def exchange(b, fills):
        for k in range(1, n_slab):
            scatter(b, k).start()
        forwards(b, 0, fills[0])
        value = part[b, pl.ds(pl.multiple_of(slab * slots, slots), slots), :]
        scattered(b).wait_recv()
        for k in range(n_slab - 1):
            value = value + landed[b, k]
        zown[b] = value
        for k in range(1, n_lev):
            along(b, k).start()
        forwards(b, fills[0], fills[0] + fills[1])
        for k in range(1, n_lev):
            along(b, k).wait_recv()
        for k in range(1, n_lev):
            value = value + zland[b, k]
        own[b] = value
        for k in range(1, n_slab):
            cast(b, k).start()
        prior[b, slab] = value
        forwards(b, fills[0] + fills[1], sum(fills))
        collected(b).wait_recv()

    def statistics(b):
        now = prior[b].reshape(n_slab * slots, LANES)
        now = jnp.concatenate([now[t * members : (t + 1) * members] for t in range(obs_tiles)], axis=1)
        value, var = value_ref[b : b + 1, :], var_ref[b : b + 1, :]
        mean = jnp.sum(now, axis=0, keepdims=True) / members
        deviation = now - mean
        spread = jnp.sum(deviation * deviation, axis=0, keepdims=True) / (members - 1.0)
        whole = spread + var
        shrink = 1.0 / (1.0 + jnp.sqrt(var / whole))
        gain = ((value - mean) - deviation * shrink) / (whole * (members - 1.0))
        pad = jnp.zeros((LANES - members, n_obs), F32)
        dev_s[...] = jnp.concatenate([deviation, pad], axis=0).T.astype(BF16)
        gain_s[...] = gain.astype(BF16)
        mean_ref[b : b + 1, :] = mean

    def spread_levels(b):
        for level in range(lev_rows):
            lev_s[level] = jnp.broadcast_to(lev_ref[b, level : level + 1, :], (LANES, n_obs)).T

    def update(b, c, span=1):
        at = pl.ds(pl.multiple_of(c * width, width), span * width)
        dev = dev_s[:, :members]
        gain = gain_s[...]
        loc = gat[b, :, at].astype(F32)
        levels = range(lev_rows)
        now = [state[level, :, at] for level in levels]
        centred = [(x - jnp.sum(x, axis=0, keepdims=True) / members).astype(BF16) for x in now]
        cross = [jnp.dot(dev, x, preferred_element_type=F32) for x in centred]
        height = [jnp.concatenate([lev_s[level]] * (span * wide), axis=1) for level in levels]
        mixed = [((height[level] * loc) * cross[level]).astype(BF16) for level in levels]
        new = [now[level] + jnp.dot(gain, mixed[level], preferred_element_type=F32) for level in levels]
        for level in levels:
            state[level, :, at] = new[level]
    acc[...] = jnp.zeros_like(acc)
    part[...] = jnp.zeros_like(part)
    for load in loads[1:]:
        load.wait()
    pltpu.make_async_copy(state, state, state_sem).wait()
    for b in range(n_blocks):
        locate(b)
    lax.fori_loop(0, chunks, pick_first, 0)
    finish_pick(0)
    for b in range(n_blocks):
        fills = STEPS_FIRST if b == 0 else STEPS_LATER
        spread_levels(b)
        exchange(b, fills)
        statistics(b)
        if b + 1 < n_blocks:
            acc[...] = jnp.zeros_like(acc)
        done = sum(fills)
        early = max(done - lag, 0)

        def advance(c):
            if b + 1 < n_blocks:
                gather(b + 1, c - 1)
            update(b, c)

        def plain(c, carry):
            advance(c)
            return carry

        def double(s, carry):
            forward(b, s)
            update(b, 2 * (s - done), 2)
            return carry

        def single(s, carry):
            forward(b, s)
            advance(s - lag)
            return carry

        if b + 1 < n_blocks:
            sent = steps - SKEW

            forwards(b, done, lag + 1)
            base = max(done, lag + 1)
            forward(b, base)
            update(b, 0)

            def between(s, carry):
                forward(b, s)
                advance(s - base)
                return carry

            lax.fori_loop(base + 1, sent, between, 0)
            send_own(b + 1)
            lax.fori_loop(sent - base, sent - lag, plain, 0)
            lax.fori_loop(sent, steps, single, 0)
            gather(b + 1, chunks - 1)
        else:
            forwards(b, done, lag)
            lax.fori_loop(lag + early, lag + 2 * early, double, 0)
            lax.fori_loop(lag + 2 * early, steps, single, 0)
        if b + 1 < n_blocks:
            finish_pick(b + 1)

    for way, step, alive in ends:
        @pl.when(alive)
        def _():
            for b in range(n_blocks):
                whole = gat.at[b, mine, :]
                pltpu.make_async_remote_copy(
                    src_ref=whole, dst_ref=whole, send_sem=own_send.at[b, way], recv_sem=line_recv.at[0, 0, 0],
                    device_id=(slab, lev + step), device_id_type=MESH).wait_send()
            for d in range(1, n_lev - 1):
                source = lev - step * d

                @pl.when((source >= 0) & (source < n_lev))
                def _():
                    for slot in range(2):
                        hop(step, 0, source, 0, line_send.at[way, d - 1, slot]).wait_send()
    for b in range(n_blocks):
        scattered(b).wait_send()
        collected(b).wait_send()
        for k in range(1, n_lev):
            along(b, k).wait_send()


def analyse(n_slab, n_lev, ensemble, cells, values, variances, fracs, locs, heights):
    members, lev_rows, cols = ensemble.shape
    n_blocks, n_obs = cells.shape
    rows = locs.shape[1]
    width = next(t * LANES for t in (2, 1) if cols % (t * LANES) == 0)
    chunks = cols // width
    packed = members * (n_obs // LANES)
    slots = pl.cdiv(packed, n_slab * SUBLANES) * SUBLANES
    vmem = pl.BlockSpec(memory_space=pltpu.VMEM)
    hbm = pl.BlockSpec(memory_space=pltpu.HBM)
    dma = pltpu.SemaphoreType.DMA
    return pl.pallas_call(
        functools.partial(kernel, n_slab, n_lev),
        out_shape=[
            pltpu.VMEM((lev_rows, members, cols), F32),
            pltpu.VMEM(values.shape, F32),
        ],
        in_specs=[hbm] * 7,
        out_specs=[vmem, vmem],
        scratch_shapes=[
            pltpu.VMEM(cells.shape, jnp.int32),
            pltpu.VMEM(fracs.shape, F32),
            pltpu.VMEM(values.shape, F32),
            pltpu.VMEM(variances.shape, F32),
            pltpu.VMEM(heights.shape, F32),
            pltpu.VMEM((n_blocks, n_obs, cols), BF16),
            pltpu.VMEM((n_blocks, 2, n_obs // LANES, 2, SUBLANES, LANES), jnp.int32),
            pltpu.VMEM((2, members, n_obs), F32),
            pltpu.VMEM((n_blocks, n_slab * slots, LANES), F32),
            pltpu.VMEM((n_blocks, n_slab - 1, slots, LANES), F32),
            pltpu.VMEM((n_blocks, slots, LANES), F32),
            pltpu.VMEM((n_blocks, n_lev, slots, LANES), F32),
            pltpu.VMEM((n_blocks, slots, LANES), F32),
            pltpu.VMEM((n_blocks, n_slab, slots, LANES), F32),
            pltpu.VMEM((n_obs, LANES), BF16),
            pltpu.VMEM((members, n_obs), BF16),
            pltpu.VMEM((lev_rows, n_obs, LANES), F32),
            dma((n_blocks + 6,)),
            dma((n_blocks, n_lev - 1, chunks)),
            dma((n_blocks, 2)),
            dma((2, n_lev - 2, 2)),
            dma((n_blocks,)),
            dma((n_blocks,)),
            dma((n_blocks, n_lev)),
            dma((n_blocks, n_lev)),
            dma((n_blocks,)),
            dma((n_blocks,)),
        ],
        compiler_params=pltpu.CompilerParams(collective_id=0, has_side_effects=True, vmem_limit_bytes=28 << 20),
        name="analyse",
    )(*(pltpu.with_memory_space_constraint(x, pltpu.HBM) for x in (cells, fracs, values, variances, heights, ensemble, locs)))


def hand_over_kernel(state, means, out_ref, mean_ref, sem):
    lev_rows = state.shape[0]
    copies = [pltpu.make_async_copy(state.at[level], out_ref.at[:, level, :], sem.at[level]) for level in range(lev_rows)]
    copies.append(pltpu.make_async_copy(means, mean_ref, sem.at[lev_rows]))
    for copy in copies:
        copy.start()
    for copy in copies:
        copy.wait()


def hand_over(state, means):
    lev_rows, members, cols = state.shape
    vmem = pl.BlockSpec(memory_space=pltpu.VMEM)
    hbm = pl.BlockSpec(memory_space=pltpu.HBM)
    return pl.pallas_call(
        hand_over_kernel,
        out_shape=[pltpu.HBM((members, lev_rows, cols), F32), pltpu.HBM(means.shape, F32)],
        in_specs=[vmem, vmem],
        out_specs=[hbm, hbm],
        scratch_shapes=[pltpu.SemaphoreType.DMA((lev_rows + 1,))],
        compiler_params=pltpu.CompilerParams(vmem_limit_bytes=8 << 20),
        name="hand_over",
    )(*(pltpu.with_memory_space_constraint(x, pltpu.VMEM) for x in (state, means)))


def solution(mesh):
    n_slab, n_lev = mesh.shape["slab"], mesh.shape["lev"]

    def on_device(ensemble, obs_cell, obs_value, obs_var, obs_frac, loc_column, loc_level):
        heights = loc_level.transpose(0, 2, 1)
        state, means = analyse(n_slab, n_lev, ensemble, obs_cell, obs_value, obs_var, obs_frac, loc_column, heights)
        return tuple(hand_over(state, means))

    in_specs = (
        P(None, "lev", "slab"), P(), P(), P(), P(),
        P(None, "lev", "slab"), P(None, None, "lev"),
    )
    return jax.shard_map(
        on_device, mesh=mesh, in_specs=in_specs,
        out_specs=(P(None, "lev", "slab"), P()), check_vma=False,
    )
```
